512 devices in a mesh: sub: 16 (over x, z_lo), blk: 32 (over z_hi, y, core).
Axes of the slice: x: 4, y: 8, z: 8 (z_hi: 2, z_lo: 4; z = z_hi * 4 + z_lo), core: 2. Of those that a mesh axis runs over, the one named last changes fastest.
Arguments:
- schur: bfloat16 [16, 8192, 8192], P('sub', 'blk'), as said below
- inverse_blocks: float32 [16, 64, 128, 128], P('sub', 'blk'), as said below
- loads: float32 [16, 32, 8192], P('sub', None, 'blk'), may hold values from -6 to 6
- share_list: int32 [16, 16, 4], P('sub'), may hold values from -1 to 63, as said below
- multiplicity: int32 [16, 64], P('sub', 'blk'), may hold values from 1 to 2, as said below
Outputs:
- solution: float32 [16, 32, 8192], P('sub', None, 'blk')
- misfit: float32 [32, 96], replicated
The draws below stay inside these ranges and needn't reach their ends.
Inputs may be any that keep to these rules, and one draw needn't show every extreme that they name: share_list[i, j, s] is the local block of subdomain i that holds the s-th block it shares with subdomain j, or -1 for an empty slot; share_list[j, i, s] is the same block in the numbering of j; the used slots of a pair come first and are as many both ways; share_list[i, i, :] is -1; no block of a subdomain appears twice in its list; at most 4 blocks a pair. multiplicity[i, k] is 2 where block k of subdomain i appears in share_list[i], else 1. `schur`: each local Schur complement is a full dense matrix. `inverse_blocks`: full dense blocks.
All inputs are finite; a program needn't handle non-finite values.
Results may differ from the reference program's by a relative error of at most 0.0026.
Values may be sent and summed in bfloat16 or wider, within the bound.
A program may use at most 64 MiB of HBM per device.

```python
import math
import jax
import jax.numpy as jnp
from jax import lax

ORDER = 8192
BLOCK = 128
SLOTS = 4
CASES = 32
ITERS = 2
NSUBS = 16
BLOCKS = 64


def interface_tables(key):
    base = jax.random.fold_in(key, 7)
    counts = jax.random.randint(jax.random.fold_in(base, 1), (NSUBS, NSUBS), 0, SLOTS + 1)
    counts = jnp.triu(counts, 1)
    counts = counts + counts.T
    busiest = jax.random.randint(jax.random.fold_in(base, 2), (), 0, NSUBS)
    ident = jnp.arange(NSUBS, dtype=jnp.int32)
    touched = (ident[:, None] == busiest) | (ident[None, :] == busiest)
    offdiag = ident[:, None] != ident[None, :]
    counts = jnp.where(touched & offdiag, SLOTS, counts)
    orders = jax.vmap(lambda which: jax.random.permutation(jax.random.fold_in(base, 100 + which), BLOCKS))(ident)
    slot_ids = jnp.arange(SLOTS, dtype=jnp.int32)
    ranked = ident[None, :] - (ident[None, :] > ident[:, None]).astype(jnp.int32)
    position = jnp.minimum(ranked[:, :, None] * SLOTS + slot_ids[None, None, :], BLOCKS - 1)
    chosen = orders[ident[:, None, None], position]
    valid = (slot_ids[None, None, :] < counts[:, :, None]) & offdiag[:, :, None]
    shared = jnp.where(valid, chosen, -1).astype(jnp.int32)
    present = jnp.any(shared[:, :, :, None] == jnp.arange(BLOCKS, dtype=jnp.int32)[None, None, None, :], axis=(1, 2))
    return (shared, (1 + present.astype(jnp.int32)).astype(jnp.int32))


def draw_share_list(key, part):
    return interface_tables(key)[0]


def draw_multiplicity(key, part):
    return interface_tables(key)[1]


def draw_schur(key, part):

    def single(which):
        sub_key = jax.random.fold_in(key, which)
        noise = jax.random.normal(sub_key, (ORDER, ORDER), jnp.float32)
        diagonal = jnp.ones((ORDER,), jnp.float32)
        symmetric = (noise + noise.T) * (0.3 / math.sqrt(2.0 * ORDER))
        return (jnp.diag(diagonal) + symmetric).astype(jnp.bfloat16)
    return lax.map(single, jnp.arange(NSUBS, dtype=jnp.int32))


def draw_inverse_blocks(key, part):
    shape = (NSUBS, BLOCKS, BLOCK, BLOCK)
    noise = jax.random.normal(key, shape, jnp.float32)
    return jnp.eye(BLOCK, dtype=jnp.float32) + noise * (0.35 / math.sqrt(BLOCK))


def level_of(stream_key, extent, pieces, least, top_value):
    factor_of = 1.0
    for axis_at, shards_of in pieces:
        steps = jax.random.uniform(jax.random.fold_in(jax.random.fold_in(stream_key, 6), axis_at), (shards_of,), jnp.float32, least / len(pieces), top_value / len(pieces))
        factor_of = factor_of * jnp.repeat(jnp.exp(steps), extent[axis_at] // shards_of).reshape((-1,) + (1,) * (len(extent) - 1 - axis_at))
    return factor_of


def centred(own_key, shape, deviation, most, shards=(), kind=jnp.bfloat16):
    factor_of = level_of(own_key, shape, shards, -0.22, 0.18) if shards else 1.0
    drawn = jax.random.normal(own_key, shape, jnp.float32) * deviation * factor_of
    return jnp.minimum(jnp.maximum(drawn, -most), most).astype(kind)


def setup_inputs(seed: int = 0) -> dict:
    keys = jax.random.split(jax.random.key(seed), 6)
    return {
        "schur": draw_schur(jax.random.fold_in(keys[5], 71), 0),
        "inverse_blocks": draw_inverse_blocks(jax.random.fold_in(keys[5], 71), 0),
        "loads": centred(keys[2], (NSUBS, CASES, ORDER), 1.0, 6.0, ((0, 16), (2, 32)), jnp.float32),
        "share_list": draw_share_list(jax.random.fold_in(keys[5], 71), 0),
        "multiplicity": draw_multiplicity(jax.random.fold_in(keys[5], 71), 0),
    }


FULL_PRECISION = lax.Precision.HIGHEST

def assemble(values, share_list):
    blocks = values.reshape(NSUBS, values.shape[1], BLOCKS, BLOCK)
    selector = (share_list[..., None] == jnp.arange(BLOCKS, dtype=jnp.int32)).astype(jnp.float32)
    outgoing = jnp.einsum('ijsk,ipkd->ijspd', selector, blocks, precision=FULL_PRECISION)
    incoming = jnp.transpose(outgoing, (1, 0, 2, 3, 4))
    summed = blocks + jnp.einsum('ijsk,ijspd->ipkd', selector, incoming, precision=FULL_PRECISION)
    return summed.reshape(values.shape)

def products(left, right, row_weight):
    weighting = 1.0 / (ORDER * NSUBS)
    return jnp.einsum('ipr,iqr->pq', left * row_weight[:, None, :], right, precision=FULL_PRECISION) * weighting

def precondition(basis, inverse_blocks, block_weight, share_list):
    blocks = basis.reshape(NSUBS, CASES, BLOCKS, BLOCK)
    local = jnp.einsum('ikde,ipke->ipkd', inverse_blocks, blocks, precision=FULL_PRECISION)
    local = local * block_weight[:, None, :, None]
    return assemble(local.reshape(NSUBS, CASES, ORDER), share_list)

def apply_schur(field, schur):
    rounded = field.astype(jnp.bfloat16)

    def single(pair):
        return lax.dot_general(pair[0].astype(jnp.float32), pair[1].astype(jnp.float32), (((1,), (1,)), ((), ())), preferred_element_type=jnp.float32)
    return lax.map(single, (rounded, schur))

def lower_solve(lower, values):
    flat = jnp.transpose(values, (1, 0, 2)).reshape(CASES, -1)
    solved = jax.scipy.linalg.solve_triangular(lower, flat, lower=True)
    return jnp.transpose(solved.reshape(CASES, NSUBS, ORDER), (1, 0, 2))

def reference(schur, inverse_blocks, loads, share_list, multiplicity):
    block_weight = 1.0 / multiplicity.astype(jnp.float32)
    row_weight = jnp.repeat(block_weight, BLOCK, axis=1)
    right_side = assemble(loads, share_list)
    first = jnp.linalg.cholesky(products(right_side, right_side, row_weight))
    basis = [lower_solve(first, right_side)]
    hessen = jnp.zeros((ITERS * CASES, (ITERS + 1) * CASES), jnp.float32)
    for level in range(ITERS):
        image = assemble(apply_schur(precondition(basis[level], inverse_blocks, block_weight, share_list), schur), share_list)
        stacked = jnp.stack(basis)
        weighting = 1.0 / (ORDER * NSUBS)
        coefs = jnp.einsum('ipr,liqr->lpq', image * row_weight[:, None, :], stacked, precision=FULL_PRECISION) * weighting
        image = image - jnp.einsum('lpq,liqr->ipr', coefs, stacked, precision=FULL_PRECISION)
        lower = jnp.linalg.cholesky(products(image, image, row_weight))
        basis.append(lower_solve(lower, image))
        rows = slice(level * CASES, (level + 1) * CASES)
        for earlier in range(level + 1):
            hessen = hessen.at[rows, earlier * CASES:(earlier + 1) * CASES].set(coefs[earlier])
        hessen = hessen.at[rows, (level + 1) * CASES:(level + 2) * CASES].set(lower)
    target = jnp.zeros((CASES, (ITERS + 1) * CASES), jnp.float32).at[:, :CASES].set(first)
    normal_matrix = jnp.dot(hessen, hessen.T, precision=FULL_PRECISION)
    right_part = jnp.dot(target, hessen.T, precision=FULL_PRECISION)
    factor = jnp.linalg.cholesky(normal_matrix)
    middle = jax.scipy.linalg.solve_triangular(factor, right_part.T, lower=True)
    coeff_t = jax.scipy.linalg.solve_triangular(factor, middle, lower=True, trans=1)
    combine = coeff_t.T
    misfit = target - jnp.dot(combine, hessen, precision=FULL_PRECISION)
    update = jnp.zeros((NSUBS, CASES, ORDER), jnp.float32)
    for level in range(ITERS):
        update = update + jnp.einsum('pq,iqr->ipr', combine[:, level * CASES:(level + 1) * CASES], basis[level], precision=FULL_PRECISION)
    solution = precondition(update, inverse_blocks, block_weight, share_list)
    return (solution, misfit)
```

```python
import functools

import jax
import jax.numpy as jnp
from jax import lax
from jax.experimental import pallas as pl
from jax.experimental.pallas import tpu as pltpu
from jax.sharding import PartitionSpec as P

MESH = pl.DeviceIdType.MESH
HIGHEST = lax.Precision.HIGHEST
NS = 16
NB = 32
CASES = 32
ROWS = 256
NN = ((1,), (0,))
NT = ((1,), (1,))
TN = ((0,), (0,))


def mm(left, right, dims):
    return lax.dot_general(
        left, right, (dims, ((), ())), precision=HIGHEST, preferred_element_type=jnp.float32
    )


def packed(field):
    return [
        jnp.concatenate(
            [field[k * 128 + q * 32 : k * 128 + q * 32 + 32, :] for q in range(4)], axis=1
        )
        for k in range(2)
    ]


def unpacked(halves):
    return jnp.concatenate(
        [halves[k][:, q * 32 : q * 32 + 32] for k in range(2) for q in range(4)], axis=0
    )


def factor(aug):
    rows_at = lax.broadcasted_iota(jnp.int32, aug.shape, 0)
    out = jnp.zeros_like(aug)
    for step in range(CASES):
        row = aug[step : step + 1, :]
        scaled = row * lax.rsqrt(row[:, step : step + 1])
        column = aug[:, step : step + 1] * lax.rsqrt(row[:, step : step + 1])
        out = jnp.where(rows_at == step, jnp.broadcast_to(scaled, aug.shape), out)
        if step < CASES - 1:
            aug = aug - column * scaled
    return out


def kernel(
    weight_ref,
    x0_ref,
    inv_send_ref,
    inv_ref,
    slot_row_ref,
    slot_col_ref,
    schur_hbm,
    sol_ref,
    misfit_ref,
    schur,
    f1_send,
    f1_recv,
    f2_send,
    f2_recv,
    f3_send,
    f3_recv,
    n1_recv,
    n2_send,
    n2_recv,
    n3_send,
    n3_recv,
    zbuf,
    basis,
    gram_buf,
    part_buf,
    ar_core,
    ar_x,
    ar_z,
    ar_y,
    ar_out,
    schur_sem,
    send_sem,
    recv_sem,
    n_send_sem,
    n_recv_sem,
    z_send_sem,
    z_recv_sem,
    ar_send_sem,
    ar_recv_sem,
):
    sub = lax.axis_index("sub")
    blk = lax.axis_index("blk")
    x, zl = sub // 4, sub % 4
    zh, y, core = blk // 16, (blk // 2) % 8, blk % 2
    z = zh * 4 + zl
    sibling = (sub, blk + 1 - 2 * core)
    other_half = (blk + 16) % NB

    load_schur = pltpu.make_async_copy(schur_hbm, schur, schur_sem)
    load_schur.start()

    def z_peer(t):
        to = (z + t) % 8
        return (x * 4 + to % 4, (to // 4) * 16 + blk % 16)

    barrier = pltpu.get_barrier_semaphore()

    def greet(device):
        pl.semaphore_signal(barrier, inc=1, device_id=device, device_id_type=MESH)

    def greet_blk(t, _):
        greet((sub, (blk + t) % NB))
        return 0

    def greet_sub(t, _):
        greet(((sub + t) % NS, blk))
        return 0

    lax.fori_loop(1, NB, greet_blk, 0)
    lax.fori_loop(1, NS, greet_sub, 0)
    def greet_z(t, _):
        greet((x * 4 + (zl + t) % 4, other_half))
        return 0

    lax.fori_loop(1, 4, greet_z, 0)

    f2_zero = jnp.zeros((3, 1, 4, 128), jnp.float32)
    f2_recv[:, pl.ds(sub, 1)] = f2_zero
    n2_recv[pl.ds(pl.multiple_of(sub * 16, 16), 16), :] = jnp.zeros((16, 128), jnp.float32)

    slot_row = slot_row_ref[...]
    slot_col = slot_col_ref[...]
    blocks_in_lanes = lax.broadcasted_iota(jnp.int32, (64, NB), 1) * 2
    blocks_in_rows = lax.broadcasted_iota(jnp.int32, (NB, 64), 0) * 2
    pick = [(slot_col == blocks_in_lanes + k).astype(jnp.float32) for k in range(2)]
    place = [(slot_row == blocks_in_rows + k).astype(jnp.float32) for k in range(2)]
    held = [1.0 / (1.0 + jnp.sum(place[k], axis=1, keepdims=True)) for k in range(2)]

    pl.semaphore_wait(barrier, NB - 1 + NS - 1 + 3)

    def remote(src, dst, send, recv, device):
        return pltpu.make_async_remote_copy(
            src_ref=src,
            dst_ref=dst,
            send_sem=send,
            recv_sem=recv,
            device_id=device,
            device_id_type=MESH,
        )

    def wait_bytes(ref, sem):
        pltpu.make_async_copy(ref, ref, sem).wait()

    def over_blk(source, target, send, recv):
        def one(t, _):
            to = (blk + 15 + t) % NB
            remote(source(to), target(blk), send, recv, (sub, to)).start()
            return 0

        lax.fori_loop(1, NB - 15, one, 0)

        def rest(t, _):
            to = (blk + t) % NB
            remote(source(to), target(blk), send, recv, (sub, to)).start()
            return 0

        lax.fori_loop(1, 16, rest, 0)

    def over_sub(source, target, send, recv):
        def one(t, _):
            to = (sub + t) % NS
            remote(source(to), target(sub), send, recv, (to, blk)).start()
            return 0

        lax.fori_loop(1, NS, one, 0)

    def eight(ref, at):
        return ref.at[pl.ds(pl.multiple_of(at * 8, 8), 8), :]

    def sixteen(ref, at):
        return ref.at[pl.ds(pl.multiple_of(at * 16, 16), 16), :]

    def scatter_rows(r, source):
        over_blk(
            lambda to: source.at[to],
            lambda own: f1_recv.at[r, own],
            send_sem.at[r, 0],
            recv_sem.at[r, 0],
        )
        f1_recv[r, pl.ds(blk, 1)] = source[pl.ds(blk, 1)]

    def exchange(r):
        wait_bytes(f1_recv.at[r, pl.ds(0, NB - 1)], recv_sem.at[r, 0])
        own = [f1_recv[r, :, k, :] for k in range(2)]
        out = mm(pick[0], own[0], NN) + mm(pick[1], own[1], NN)
        for j in range(NS):
            f2_send[r, j] = out[4 * j : 4 * j + 4, :]
        over_sub(
            lambda to: f2_send.at[r, to],
            lambda own_sub: f2_recv.at[r, own_sub],
            send_sem.at[r, 1],
            recv_sem.at[r, 1],
        )
        return own

    def assembled(r, own):
        wait_bytes(f2_recv.at[r, pl.ds(0, NS - 1)], recv_sem.at[r, 1])
        came = jnp.concatenate([f2_recv[r, j] for j in range(NS)], axis=0)
        return [own[k] + mm(place[k], came, NN) for k in range(2)]

    def gather_rows(r, halves):
        for k in range(2):
            f3_send[r, :, k, :] = halves[k]
        over_blk(
            lambda to: f3_send.at[r, to],
            lambda own: f3_recv.at[r, own],
            send_sem.at[r, 2],
            recv_sem.at[r, 2],
        )
        f3_recv[r, pl.ds(blk, 1)] = f3_send[r, pl.ds(blk, 1)]

    def owned_rows(r):
        wait_bytes(f3_recv.at[r, pl.ds(0, NB - 1)], recv_sem.at[r, 2])
        return unpacked([f3_recv[r, :, k, :] for k in range(2)])

    def gram(r, halves):
        stacked = unpacked(halves)
        basis[:, r * 32 : r * 32 + 32] = stacked
        weighted = unpacked([halves[k] * held[k] for k in range(2)])
        return mm(weighted, basis[...], TN) * (1.0 / (NS * NB * ROWS))

    def all_reduce(r, local):
        gram_buf[r] = local
        remote(
            gram_buf.at[r, pl.ds(pl.multiple_of((1 - core) * 16, 16), 16), :],
            ar_core.at[r],
            ar_send_sem.at[r, 0],
            ar_recv_sem.at[r, 0],
            sibling,
        ).start()
        yield
        wait_bytes(ar_core.at[r], ar_recv_sem.at[r, 0])
        mine = gram_buf[r, pl.ds(pl.multiple_of(core * 16, 16), 16), :]
        came = ar_core[r]
        value = mine + came
        for phase, (buf, count, at, peer) in enumerate(
            (
                (ar_x, 4, x, lambda t: (((x + t) % 4) * 4 + zl, blk)),
                (ar_z, 8, z, z_peer),
                (ar_y, 8, y, lambda t: (sub, zh * 16 + ((y + t) % 8) * 2 + core)),
            )
        ):
            buf[r, pl.ds(at, 1)] = value[None]
            part_buf[r, phase] = value

            def one(t, _, buf=buf, at=at, peer=peer, phase=phase):
                remote(
                    part_buf.at[r, phase],
                    buf.at[r, at],
                    ar_send_sem.at[r, phase + 1],
                    ar_recv_sem.at[r, phase + 1],
                    peer(t),
                ).start()
                return 0

            lax.fori_loop(1, count, one, 0)
            yield
            wait_bytes(buf.at[r, pl.ds(0, count - 1)], ar_recv_sem.at[r, phase + 1])
            value = buf[r, 0]
            for t in range(1, count):
                value = value + buf[r, t]
        own_half = pl.ds(pl.multiple_of(core * 16, 16), 16)
        ar_out[r, own_half, :] = value
        part_buf[r, 3] = value
        remote(
            part_buf.at[r, 3],
            ar_out.at[r, own_half, :],
            ar_send_sem.at[r, 4],
            ar_recv_sem.at[r, 4],
            sibling,
        ).start()
        yield
        wait_bytes(ar_out.at[r, pl.ds(0, 16), :], ar_recv_sem.at[r, 4])
        yield

    def drain(steps):
        for _ in steps:
            pass

    def columns(r, device):
        return zbuf.at[r, :, pl.ds(pl.multiple_of(device * ROWS, ROWS), ROWS)]

    def pass_on(r, chunk, device):
        remote(
            columns(r, chunk), columns(r, chunk), z_send_sem.at[r], z_recv_sem.at[r, chunk], device
        ).start()

    def arrived(r, chunk):
        wait_bytes(columns(r, chunk), z_recv_sem.at[r, chunk])

    def along_y(r, chunk):
        def one(t, _):
            pass_on(r, chunk, (sub, zh * 16 + ((y + t) % 8) * 2 + core))
            return 0

        lax.fori_loop(1, 8, one, 0)

    def apply_schur(r, field, meanwhile):
        zbuf[r, :, pl.ds(pl.multiple_of(blk * ROWS, ROWS), ROWS)] = jnp.transpose(field).astype(
            jnp.bfloat16
        )
        pass_on(r, blk, (sub, other_half))
        along_y(r, blk)
        pass_on(r, blk, sibling)
        next(meanwhile, None)

        def to_sibling(base):
            def one(t, _):
                away = (t + 1) // 2 + (t % 2 - 1) * (2 * ((t + 1) // 2) - 8)
                chunk = base * 16 + ((y + away) % 8) * 2 + core
                arrived(r, chunk)
                pass_on(r, chunk, sibling)
                return 0

            return one

        def from_sibling(base):
            def one(t, _):
                arrived(r, base * 16 + ((y + t) % 8) * 2 + 1 - core)
                return 0

            return one

        lax.fori_loop(1, 5, to_sibling(zh), 0)
        arrived(r, other_half)
        along_y(r, other_half)
        pass_on(r, other_half, sibling)
        lax.fori_loop(5, 8, to_sibling(zh), 0)
        lax.fori_loop(0, 8, from_sibling(zh), 0)
        next(meanwhile, None)
        if r == 0:
            load_schur.wait()
        near = pl.ds(pl.multiple_of(zh * 4096, 4096), 4096)
        far = pl.ds(pl.multiple_of((1 - zh) * 4096, 4096), 4096)
        total = lax.dot_general(
            schur[:, near], zbuf[r, :, near], (NT, ((), ())), preferred_element_type=jnp.float32
        )
        next(meanwhile, None)
        lax.fori_loop(1, 8, to_sibling(1 - zh), 0)
        next(meanwhile, None)
        lax.fori_loop(0, 8, from_sibling(1 - zh), 0)
        return total + lax.dot_general(
            schur[:, far], zbuf[r, :, far], (NT, ((), ())), preferred_element_type=jnp.float32
        )

    def precondition(blocks, field):
        return jnp.concatenate(
            [mm(blocks[k], field[k * 128 : k * 128 + 128, :], NN) for k in range(2)], axis=0
        )

    identity = (
        lax.broadcasted_iota(jnp.int32, (CASES, CASES), 0)
        == lax.broadcasted_iota(jnp.int32, (CASES, CASES), 1)
    ).astype(jnp.float32)
    blank = jnp.zeros((CASES, CASES), jnp.float32)

    def with_right(matrix, *right):
        filled = (matrix, *right) + (blank,) * (3 - len(right))
        return jnp.concatenate(filled, axis=1)

    basis[...] = jnp.zeros((ROWS, 128), jnp.float32)
    scatter_rows(0, x0_ref)
    over_blk(
        lambda to: eight(inv_send_ref, to),
        lambda own: eight(n1_recv, own),
        n_send_sem.at[0],
        n_recv_sem.at[0],
    )
    n1_recv[pl.ds(pl.multiple_of(blk * 8, 8), 8), :] = inv_send_ref[
        pl.ds(pl.multiple_of(blk * 8, 8), 8), :
    ]
    own = exchange(0)
    wait_bytes(n1_recv.at[pl.ds(0, 248), :], n_recv_sem.at[0])
    for q in range(4):
        out = mm(pick[0], n1_recv[pl.ds(q, NB, stride=8), :], NN) + mm(
            pick[1], n1_recv[pl.ds(4 + q, NB, stride=8), :], NN
        )
        for j in range(NS):
            n2_send[j * 16 + q * 4 : j * 16 + q * 4 + 4, :] = out[4 * j : 4 * j + 4, :]
    over_sub(
        lambda to: sixteen(n2_send, to),
        lambda own_sub: sixteen(n2_recv, own_sub),
        n_send_sem.at[1],
        n_recv_sem.at[1],
    )
    right_side = assembled(0, own)
    gather_rows(0, right_side)
    first_sum = all_reduce(0, gram(0, right_side))
    next(first_sum)
    wait_bytes(n2_recv.at[pl.ds(0, 240), :], n_recv_sem.at[1])
    for q in range(4):
        came = jnp.concatenate(
            [n2_recv[j * 16 + q * 4 : j * 16 + q * 4 + 4, :] for j in range(NS)], axis=0
        )
        for k in range(2):
            n3_send[pl.ds(k * 4 + q, NB, stride=8), :] = mm(place[k], came, NN)
    over_blk(
        lambda to: eight(n3_send, to),
        lambda own: eight(n3_recv, own),
        n_send_sem.at[2],
        n_recv_sem.at[2],
    )
    n3_recv[pl.ds(pl.multiple_of(blk * 8, 8), 8), :] = n3_send[
        pl.ds(pl.multiple_of(blk * 8, 8), 8), :
    ]
    drain(first_sum)
    start = factor(with_right(ar_out[0][:, :32], identity))
    c0_t, c0_inv = start[:, :32], start[:, 32:64]
    v0 = mm(owned_rows(0), c0_inv, NT)
    wait_bytes(n3_recv.at[pl.ds(0, 248), :], n_recv_sem.at[2])
    blocks = [
        (
            inv_ref[k * 128 : k * 128 + 128, :]
            + jnp.concatenate(
                [n3_recv[pl.ds(k * 4 + q, NB, stride=8), :] for q in range(4)], axis=0
            )
        )
        * weight_ref[0, k]
        for k in range(2)
    ]
    mv0 = precondition(blocks, v0)

    w0 = apply_schur(0, mv0, iter(()))
    for k, half in enumerate(packed(w0)):
        f1_send[0, :, k, :] = half
    scatter_rows(1, f1_send.at[0])
    own = exchange(1)
    image = assembled(1, own)
    gather_rows(1, image)
    second_sum = all_reduce(1, gram(1, image))
    next(second_sum)
    z1 = precondition(blocks, owned_rows(1))
    next(second_sum)

    y1 = apply_schur(1, z1, second_sum)
    drain(second_sum)
    sums = ar_out[1]
    h00 = mm(sums[:, :32], c0_inv, NT)
    w0w0 = sums[:, 32:64]
    low = factor(with_right(w0w0 - mm(h00, h00, NT), identity))
    h10_t, h10_inv = low[:, :32], low[:, 32:64]
    w1 = mm(y1 - mm(w0, h00, NT), h10_inv, NT)
    for k, half in enumerate(packed(w1)):
        f1_send[1, :, k, :] = half
    scatter_rows(2, f1_send.at[1])
    h00_c0 = mm(h00, c0_t, NN)
    fact = factor(with_right(w0w0, identity, h00_c0))
    f_inv_low, f_right = fact[:, 32:64], fact[:, 64:96]
    f_inv = mm(f_inv_low, f_inv_low, TN)
    own = exchange(2)
    mv1 = mm(z1 - mm(mv0, h00, NT), h10_inv, NT)
    last = gram(2, assembled(2, own))
    drain(all_reduce(2, last))
    sums = ar_out[2]
    h01 = mm(sums[:, :32], c0_inv, NT)
    g21 = sums[:, 32:64]
    w1w1 = sums[:, 64:96]
    h11 = mm(g21 - mm(h01, h00, NT), h10_inv, NT)
    a1 = mm(f_inv_low, g21, NT)
    right = mm(h01, c0_t, NN) - mm(a1, f_right, TN)
    solved = factor(with_right(w1w1 - mm(a1, a1, TN), identity, right))
    h21_t = factor(with_right(w1w1 - mm(h01, h01, NT) - mm(h11, h11, NT)))[:, :32]
    y_1 = mm(solved[:, 64:96], solved[:, 32:64], TN)
    r0 = mm(c0_t, h00, ((0,), (1,)))
    y_0 = mm(r0 - mm(y_1, g21, NN), f_inv, NN)
    sol_ref[...] = mm(y_0, mv0, NT) + mm(y_1, mv1, NT)
    c0 = mm(c0_t, identity, TN)
    misfit_ref[:, :32] = c0 - mm(y_0, h00, NN) - mm(y_1, h01, NN)
    misfit_ref[:, 32:64] = -mm(y_0, h10_t, NT) - mm(y_1, h11, NN)
    misfit_ref[:, 64:96] = -mm(y_1, h21_t, NT)

    for r in range(3):
        wait_bytes(f1_recv.at[r, pl.ds(0, NB - 1)], send_sem.at[r, 0])
        wait_bytes(f2_recv.at[r, pl.ds(0, NS - 1)], send_sem.at[r, 1])
        if r < 2:
            wait_bytes(f3_recv.at[r, pl.ds(0, NB - 1)], send_sem.at[r, 2])
            wait_bytes(zbuf.at[r, :, pl.ds(0, 31 * ROWS)], z_send_sem.at[r])
        wait_bytes(ar_core.at[r], ar_send_sem.at[r, 0])
        wait_bytes(ar_x.at[r, pl.ds(0, 3)], ar_send_sem.at[r, 1])
        wait_bytes(ar_z.at[r, pl.ds(0, 7)], ar_send_sem.at[r, 2])
        wait_bytes(ar_y.at[r, pl.ds(0, 7)], ar_send_sem.at[r, 3])
        wait_bytes(ar_core.at[r], ar_send_sem.at[r, 4])
    wait_bytes(n1_recv.at[pl.ds(0, 248), :], n_send_sem.at[0])
    wait_bytes(n2_recv.at[pl.ds(0, 240), :], n_send_sem.at[1])
    wait_bytes(n1_recv.at[pl.ds(0, 248), :], n_send_sem.at[2])


def body(schur, inverse_blocks, loads, share_list, multiplicity):
    weight = 1.0 / multiplicity.astype(jnp.float32)
    x0 = jnp.transpose(loads[0].reshape(CASES, 2, 4, 32), (3, 1, 2, 0)).reshape(32, 2, 128)
    inverse = inverse_blocks[0]
    inv_send = jnp.transpose(inverse.reshape(2, 4, 32, 128), (2, 0, 1, 3)).reshape(256, 128)
    slots = share_list[0].reshape(1, 64)
    f32 = jnp.float32
    vmem = pl.BlockSpec(memory_space=pltpu.VMEM)
    dma = pltpu.SemaphoreType.DMA
    sol, misfit = pl.pallas_call(
        kernel,
        out_shape=(
            jax.ShapeDtypeStruct((CASES, ROWS), f32),
            jax.ShapeDtypeStruct((CASES, 96), f32),
        ),
        in_specs=[pl.BlockSpec(memory_space=pltpu.SMEM)]
        + [vmem] * 5
        + [pl.BlockSpec(memory_space=pl.ANY)],
        out_specs=(vmem, vmem),
        scratch_shapes=[
            pltpu.VMEM((256, 8192), jnp.bfloat16),
            pltpu.VMEM((2, NB, 2, 128), f32),
            pltpu.VMEM((3, NB, 2, 128), f32),
            pltpu.VMEM((3, NS, 4, 128), f32),
            pltpu.VMEM((3, NS, 4, 128), f32),
            pltpu.VMEM((2, NB, 2, 128), f32),
            pltpu.VMEM((2, NB, 2, 128), f32),
            pltpu.VMEM((256, 128), f32),
            pltpu.VMEM((256, 128), f32),
            pltpu.VMEM((256, 128), f32),
            pltpu.VMEM((256, 128), f32),
            pltpu.VMEM((256, 128), f32),
            pltpu.VMEM((2, CASES, 8192), jnp.bfloat16),
            pltpu.VMEM((256, 128), f32),
            pltpu.VMEM((3, 32, 128), f32),
            pltpu.VMEM((3, 4, 16, 128), f32),
            pltpu.VMEM((3, 16, 128), f32),
            pltpu.VMEM((3, 4, 16, 128), f32),
            pltpu.VMEM((3, 8, 16, 128), f32),
            pltpu.VMEM((3, 8, 16, 128), f32),
            pltpu.VMEM((3, 32, 128), f32),
            dma,
            dma((3, 3)),
            dma((3, 3)),
            dma((3,)),
            dma((3,)),
            dma((2,)),
            dma((2, NB)),
            dma((3, 5)),
            dma((3, 5)),
        ],
        compiler_params=pltpu.CompilerParams(collective_id=0, has_side_effects=True),
    )(
        weight,
        x0,
        inv_send,
        inverse.reshape(256, 128),
        slots,
        slots.reshape(64, 1),
        schur[0],
    )
    return sol[None], misfit


def solution(mesh):
    placed = (
        P("sub", "blk", None),
        P("sub", "blk", None, None),
        P("sub", None, "blk"),
        P("sub", None, None),
        P("sub", "blk"),
    )
    return jax.shard_map(
        body, mesh=mesh, in_specs=placed, out_specs=(P("sub", None, "blk"), P()), check_vma=False
    )
```

```python
import functools

import jax
import jax.numpy as jnp
from jax import lax
from jax.experimental import pallas as pl
from jax.experimental.pallas import tpu as pltpu
from jax.sharding import PartitionSpec as P

MESH = pl.DeviceIdType.MESH
HIGHEST = lax.Precision.HIGHEST
NS = 16
NB = 32
CASES = 32
ROWS = 256
NN = ((1,), (0,))
NT = ((1,), (1,))
TN = ((0,), (0,))


def mm(left, right, dims):
    return lax.dot_general(
        left, right, (dims, ((), ())), precision=HIGHEST, preferred_element_type=jnp.float32
    )


def packed(field):
    return [
        jnp.concatenate(
            [field[k * 128 + q * 32 : k * 128 + q * 32 + 32, :] for q in range(4)], axis=1
        )
        for k in range(2)
    ]


def unpacked(halves):
    return jnp.concatenate(
        [halves[k][:, q * 32 : q * 32 + 32] for k in range(2) for q in range(4)], axis=0
    )


def factor(*augs):
    augs = list(augs)
    done = [[] for _ in augs]
    lanes = (1, 128)
    for first in range(0, CASES, 4):
        for which, aug in enumerate(augs):
            rows = [aug[first + i : first + i + 1, :] for i in range(4)]
            spot = {
                (i, k): jnp.broadcast_to(rows[i][:, first + k : first + k + 1], lanes)
                for i in range(4)
                for k in range(i + 1)
            }
            columns = [
                jnp.broadcast_to(aug[:, first + i : first + i + 1], aug.shape) for i in range(4)
            ]
            low, scale = {}, []
            for i in range(4):
                for k in range(i):
                    value = spot[i, k]
                    for m in range(k):
                        value = value - low[i, m] * low[k, m]
                    low[i, k] = value * scale[k]
                value = spot[i, i]
                for m in range(i):
                    value = value - low[i, m] * low[i, m]
                scale.append(lax.rsqrt(value))
            for i in range(4):
                for m in range(i):
                    rows[i] = rows[i] - low[i, m] * rows[m]
                    columns[i] = columns[i] - low[i, m] * columns[m]
                rows[i] = rows[i] * scale[i]
                columns[i] = columns[i] * scale[i]
            done[which] += rows
            if first + 4 < CASES:
                for i in range(4):
                    aug = aug - columns[i] * rows[i]
                augs[which] = aug
    return [jnp.concatenate(rows, axis=0) for rows in done]


def folded(grams):
    return jnp.concatenate(
        [
            jnp.concatenate([gram[8 * i : 8 * i + 8, :] for i in range(4)], axis=1)
            for gram in grams
        ],
        axis=0,
    )


def unfolded(rows):
    return [
        jnp.concatenate([rows[8 * g : 8 * g + 8, 32 * i : 32 * i + 32] for i in range(4)], axis=0)
        for g in range(rows.shape[0] // 8)
    ]


def kernel(
    multiplicity_ref,
    share_ref,
    loads_hbm,
    inv_hbm,
    schur_hbm,
    sol_ref,
    misfit_ref,
    schur,
    f1_send,
    f1_recv,
    f2_send,
    f2_recv,
    f3_send,
    f3_recv,
    n1_send,
    n1_recv,
    n2_send,
    n2_recv,
    n3_send,
    n3_recv,
    zbuf,
    product,
    loads_buf,
    inv_buf,
    part_buf,
    ar_x,
    ar_z,
    ar_y,
    ar_core,
    schur_sem,
    input_sem,
    send_sem,
    recv_sem,
    n_send_sem,
    n_recv_sem,
    z_send_sem,
    z_recv_sem,
    ar_send_sem,
    ar_recv_sem,
):
    sub = lax.axis_index("sub")
    blk = lax.axis_index("blk")
    x, zl = sub // 4, sub % 4
    zh, y, core = blk // 16, (blk // 2) % 8, blk % 2
    z = zh * 4 + zl
    sibling = (sub, blk + 1 - 2 * core)
    other_half = (blk + 16) % NB

    load_loads = pltpu.make_async_copy(loads_hbm, loads_buf, input_sem.at[0])
    load_loads.start()
    load_inv = pltpu.make_async_copy(inv_hbm, inv_buf, input_sem.at[1])
    load_inv.start()

    def z_peer(t):
        to = (z + t) % 8
        return (x * 4 + to % 4, (to // 4) * 16 + blk % 16)

    barrier = pltpu.get_barrier_semaphore()

    def greet(device):
        pl.semaphore_signal(barrier, inc=1, device_id=device, device_id_type=MESH)

    def greet_blk(t, _):
        greet((sub, (blk + 15 + t) % NB))
        return 0

    def greet_near(t, _):
        greet((sub, (blk + t) % NB))
        return 0

    def greet_sub(t, _):
        greet(((sub + t) % NS, blk))
        return 0

    def greet_z(t, _):
        greet((x * 4 + (zl + t) % 4, other_half))
        return 0

    lax.fori_loop(1, NB - 15, greet_blk, 0)
    lax.fori_loop(1, 4, greet_z, 0)
    lax.fori_loop(1, 16, greet_near, 0)
    lax.fori_loop(1, NS, greet_sub, 0)

    def load_columns(chunk, _):
        at = (chunk // 16) * 16 + (chunk % 2) * 8 + (chunk // 2) % 8
        pltpu.make_async_copy(
            schur_hbm.at[:, pl.ds(pl.multiple_of(chunk * ROWS, ROWS), ROWS)],
            schur.at[:, pl.ds(pl.multiple_of(at * ROWS, ROWS), ROWS)],
            schur_sem,
        ).start()
        return 0

    lax.fori_loop(0, NB, load_columns, 0)

    f2_zero = jnp.zeros((3, 1, 4, 128), jnp.float32)
    f2_recv[:, pl.ds(sub, 1)] = f2_zero
    n2_recv[pl.ds(pl.multiple_of(sub * 16, 16), 16), :] = jnp.zeros((16, 128), jnp.float32)

    slot_at = lax.broadcasted_iota(jnp.int32, (NB, 64), 1)
    slots = jnp.full((NB, 64), -1, jnp.int32)
    for m in range(64):
        slots = jnp.where(slot_at == m, share_ref[0, m // 4, m % 4], slots)
    block_at = lax.broadcasted_iota(jnp.int32, (NB, 64), 0) * 2
    place = [(slots == block_at + k).astype(jnp.float32) for k in range(2)]
    pick = [jnp.transpose(place[k]) for k in range(2)]
    held = [1.0 / (1.0 + jnp.sum(place[k], axis=1, keepdims=True)) for k in range(2)]

    load_loads.wait()
    for k, half in enumerate(packed(jnp.transpose(loads_buf[0]))):
        f1_send[0, :, k, :] = half
    load_inv.wait()
    for k in range(2):
        for q in range(4):
            n1_send[pl.ds(k * 4 + q, NB, stride=8), :] = inv_buf[0, k, q * 32 : q * 32 + 32, :]

    pl.semaphore_wait(barrier, NB - 1 + NS - 1 + 3)

    def remote(src, dst, send, recv, device):
        return pltpu.make_async_remote_copy(
            src_ref=src,
            dst_ref=dst,
            send_sem=send,
            recv_sem=recv,
            device_id=device,
            device_id_type=MESH,
        )

    def wait_bytes(ref, sem):
        pltpu.make_async_copy(ref, ref, sem).wait()

    def over_blk(source, target, send, recv):
        def one(t, _):
            to = (blk + 15 + t) % NB
            remote(source(to), target(blk), send, recv, (sub, to)).start()
            return 0

        lax.fori_loop(1, NB - 15, one, 0)

        def rest(t, _):
            to = (blk + t) % NB
            remote(source(to), target(blk), send, recv, (sub, to)).start()
            return 0

        lax.fori_loop(1, 16, rest, 0)

    def over_sub(source, target, send, recv):
        def one(t, _):
            to = (sub + t) % NS
            remote(source(to), target(sub), send, recv, (to, blk)).start()
            return 0

        lax.fori_loop(1, NS, one, 0)

    def eight(ref, at):
        return ref.at[pl.ds(pl.multiple_of(at * 8, 8), 8), :]

    def sixteen(ref, at):
        return ref.at[pl.ds(pl.multiple_of(at * 16, 16), 16), :]

    def scatter_rows(r, source):
        over_blk(
            lambda to: source.at[to],
            lambda own: f1_recv.at[r, own],
            send_sem.at[r, 0],
            recv_sem.at[r, 0],
        )
        f1_recv[r, pl.ds(blk, 1)] = source[pl.ds(blk, 1)]

    def exchange(r):
        wait_bytes(f1_recv.at[r, pl.ds(0, NB - 1)], recv_sem.at[r, 0])
        own = [f1_recv[r, :, k, :] for k in range(2)]
        out = mm(pick[0], own[0], NN) + mm(pick[1], own[1], NN)
        for j in range(NS):
            f2_send[r, j] = out[4 * j : 4 * j + 4, :]
        over_sub(
            lambda to: f2_send.at[r, to],
            lambda own_sub: f2_recv.at[r, own_sub],
            send_sem.at[r, 1],
            recv_sem.at[r, 1],
        )
        return own

    def assembled(r, own):
        wait_bytes(f2_recv.at[r, pl.ds(0, NS - 1)], recv_sem.at[r, 1])
        came = jnp.concatenate([f2_recv[r, j] for j in range(NS)], axis=0)
        return [own[k] + mm(place[k], came, NN) for k in range(2)]

    def gather_rows(r, halves):
        for k in range(2):
            f3_send[r, :, k, :] = halves[k]
        over_blk(
            lambda to: f3_send.at[r, to],
            lambda own: f3_recv.at[r, own],
            send_sem.at[r, 2],
            recv_sem.at[r, 2],
        )
        f3_recv[r, pl.ds(blk, 1)] = f3_send[r, pl.ds(blk, 1)]

    def owned_rows(r):
        wait_bytes(f3_recv.at[r, pl.ds(0, NB - 1)], recv_sem.at[r, 2])
        return unpacked([f3_recv[r, :, k, :] for k in range(2)])

    def stacked(halves):
        weighted = unpacked([halves[k] * held[k] for k in range(2)])
        return weighted, unpacked(halves)

    def grams(left, *rights):
        scale = 1.0 / (NS * NB * ROWS)
        return folded([mm(left, right, TN) * scale for right in rights])

    def all_reduce(r, value):
        rows = value.shape[0]
        used = pl.ds(0, rows)
        for phase, (buf, count, at, peer) in enumerate(
            (
                (ar_x, 4, x, lambda t: (((x + t) % 4) * 4 + zl, blk)),
                (ar_z, 8, z, z_peer),
                (ar_y, 8, y, lambda t: (sub, zh * 16 + ((y + t) % 8) * 2 + core)),
                (ar_core, 2, core, lambda t: sibling),
            )
        ):
            part_buf[r, phase, :rows] = value
            buf[r, pl.ds(at, 1), :rows] = value[None]

            def one(t, _, buf=buf, at=at, peer=peer, phase=phase):
                remote(
                    part_buf.at[r, phase, used],
                    buf.at[r, at, used],
                    ar_send_sem.at[r, phase],
                    ar_recv_sem.at[r, phase],
                    peer(t),
                ).start()
                return 0

            lax.fori_loop(1, count, one, 0)
            yield None
            wait_bytes(buf.at[r, pl.ds(0, count - 1), used], ar_recv_sem.at[r, phase])
            value = buf[r, 0, :rows]
            for t in range(1, count):
                value = value + buf[r, t, :rows]
        result = unfolded(value)
        while True:
            yield result

    def drain(steps):
        while (result := next(steps)) is None:
            pass
        return result

    def columns(r, at):
        return zbuf.at[r, :, pl.ds(pl.multiple_of(at * ROWS, ROWS), ROWS)]

    def pass_on(r, at, device):
        remote(
            columns(r, at), columns(r, at), z_send_sem.at[r], z_recv_sem.at[r, at], device
        ).start()

    def arrived(r, at):
        wait_bytes(columns(r, at), z_recv_sem.at[r, at])

    def along_y(r, at):
        def one(t, _):
            pass_on(r, at, (sub, zh * 16 + ((y + t) % 8) * 2 + core))
            return 0

        lax.fori_loop(1, 8, one, 0)

    def apply_schur(r, field, meanwhile):
        mine = zh * 16 + core * 8
        far_mine = (1 - zh) * 16 + core * 8
        zbuf[r, :, pl.ds(pl.multiple_of((mine + y) * ROWS, ROWS), ROWS)] = jnp.transpose(
            field
        ).astype(jnp.bfloat16)
        pass_on(r, mine + y, (sub, other_half))
        along_y(r, mine + y)
        pass_on(r, mine + y, sibling)
        next(meanwhile, None)

        def to_sibling(base):
            def one(t, _):
                away = (t + 1) // 2 + (t % 2 - 1) * (2 * ((t + 1) // 2) - 8)
                at = base + (y + away) % 8
                arrived(r, at)
                pass_on(r, at, sibling)
                return 0

            return one

        def from_sibling(base):
            def one(t, _):
                arrived(r, base + (y + t) % 8)
                return 0

            return one

        def multiply(base, fresh=False):
            part = pl.ds(pl.multiple_of(base * ROWS, 2048), 2048)
            term = lax.dot_general(
                schur[:, part], zbuf[r, :, part], (NT, ((), ())), preferred_element_type=jnp.float32
            )
            return term if fresh else product[...] + term

        lax.fori_loop(1, 5, to_sibling(mine), 0)
        arrived(r, far_mine + y)
        along_y(r, far_mine + y)
        pass_on(r, far_mine + y, sibling)
        lax.fori_loop(5, 8, to_sibling(mine), 0)
        if r == 0:
            wait_bytes(schur, schur_sem)
        product[...] = multiply(mine, True)
        next(meanwhile, None)
        lax.fori_loop(0, 8, from_sibling(zh * 16 + (1 - core) * 8), 0)
        product[...] = multiply(zh * 16 + (1 - core) * 8)
        next(meanwhile, None)
        lax.fori_loop(1, 8, to_sibling(far_mine), 0)
        product[...] = multiply(far_mine)
        next(meanwhile, None)
        lax.fori_loop(0, 8, from_sibling((1 - zh) * 16 + (1 - core) * 8), 0)
        return multiply((1 - zh) * 16 + (1 - core) * 8)

    def precondition(blocks, field):
        return jnp.concatenate(
            [mm(blocks[k], field[k * 128 : k * 128 + 128, :], NN) for k in range(2)], axis=0
        )

    identity = (
        lax.broadcasted_iota(jnp.int32, (CASES, CASES), 0)
        == lax.broadcasted_iota(jnp.int32, (CASES, CASES), 1)
    ).astype(jnp.float32)
    blank = jnp.zeros((CASES, CASES), jnp.float32)

    def with_right(matrix, *right):
        filled = (matrix, *right) + (blank,) * (3 - len(right))
        return jnp.concatenate(filled, axis=1)

    scatter_rows(0, f1_send.at[0])
    over_blk(
        lambda to: eight(n1_send, to),
        lambda own: eight(n1_recv, own),
        n_send_sem.at[0],
        n_recv_sem.at[0],
    )
    n1_recv[pl.ds(pl.multiple_of(blk * 8, 8), 8), :] = n1_send[
        pl.ds(pl.multiple_of(blk * 8, 8), 8), :
    ]
    own = exchange(0)
    wait_bytes(n1_recv.at[pl.ds(0, 248), :], n_recv_sem.at[0])
    for q in range(4):
        out = mm(pick[0], n1_recv[pl.ds(q, NB, stride=8), :], NN) + mm(
            pick[1], n1_recv[pl.ds(4 + q, NB, stride=8), :], NN
        )
        for j in range(NS):
            n2_send[j * 16 + q * 4 : j * 16 + q * 4 + 4, :] = out[4 * j : 4 * j + 4, :]
    over_sub(
        lambda to: sixteen(n2_send, to),
        lambda own_sub: sixteen(n2_recv, own_sub),
        n_send_sem.at[1],
        n_recv_sem.at[1],
    )
    right_side = assembled(0, own)
    gather_rows(0, right_side)
    first_sum = all_reduce(0, grams(*stacked(right_side)))
    next(first_sum)
    wait_bytes(n2_recv.at[pl.ds(0, 240), :], n_recv_sem.at[1])
    for q in range(4):
        came = jnp.concatenate(
            [n2_recv[j * 16 + q * 4 : j * 16 + q * 4 + 4, :] for j in range(NS)], axis=0
        )
        for k in range(2):
            n3_send[pl.ds(k * 4 + q, NB, stride=8), :] = mm(place[k], came, NN)
    over_blk(
        lambda to: eight(n3_send, to),
        lambda own: eight(n3_recv, own),
        n_send_sem.at[2],
        n_recv_sem.at[2],
    )
    n3_recv[pl.ds(pl.multiple_of(blk * 8, 8), 8), :] = n3_send[
        pl.ds(pl.multiple_of(blk * 8, 8), 8), :
    ]
    (b_gram,) = drain(first_sum)
    (start,) = factor(with_right(b_gram, identity))
    c0_t, c0_inv = start[:, :32], start[:, 32:64]
    b_rows = owned_rows(0)
    v0 = mm(b_rows, c0_inv, NT)
    wait_bytes(n3_recv.at[pl.ds(0, 248), :], n_recv_sem.at[2])
    blocks = [
        (
            inv_buf[0, k]
            + jnp.concatenate(
                [n3_recv[pl.ds(k * 4 + q, NB, stride=8), :] for q in range(4)], axis=0
            )
        )
        * (1.0 / jnp.full((1, 128), multiplicity_ref[0, k].astype(jnp.float32)))
        for k in range(2)
    ]
    mv0 = precondition(blocks, v0)

    w0 = apply_schur(0, mv0, iter(()))
    for k, half in enumerate(packed(w0)):
        f1_send[1, :, k, :] = half
    scatter_rows(1, f1_send.at[1])
    own = exchange(1)
    image = assembled(1, own)
    gather_rows(1, image)
    weighted, plain = stacked(image)
    second_sum = all_reduce(1, grams(weighted, stacked(right_side)[1], plain))
    next(second_sum)
    w0_rows = owned_rows(1)
    z1 = precondition(blocks, w0_rows)
    next(second_sum)

    y1 = apply_schur(1, z1, second_sum)
    w0b, w0w0 = drain(second_sum)
    h00 = mm(w0b, c0_inv, NT)
    (low,) = factor(with_right(w0w0 - mm(h00, h00, NT), identity))
    h10_t, h10_inv = low[:, :32], low[:, 32:64]
    w1 = mm(y1 - mm(w0, h00, NT), h10_inv, NT)
    for k, half in enumerate(packed(w1)):
        f1_send[2, :, k, :] = half
    scatter_rows(2, f1_send.at[2])
    third_sum = all_reduce(2, grams(w1, b_rows, w0_rows))
    next(third_sum)
    h00_c0 = mm(h00, c0_t, NN)
    (fact,) = factor(with_right(w0w0, identity, h00_c0))
    f_inv_low, f_right = fact[:, 32:64], fact[:, 64:96]
    f_inv = mm(f_inv_low, f_inv_low, TN)
    own = exchange(2)
    next(third_sum)
    mv1 = mm(z1 - mm(mv0, h00, NT), h10_inv, NT)
    c0 = mm(c0_t, identity, TN)
    r0_f = mm(mm(c0_t, h00, ((0,), (1,))), f_inv, NN)
    sol_base = mm(r0_f, mv0, NT)
    misfit_base = (c0 - mm(r0_f, h00, NN), -mm(r0_f, h10_t, NT))
    last_sum = all_reduce(3, grams(*stacked(assembled(2, own))))
    next(last_sum)
    next(third_sum)
    next(last_sum)
    next(third_sum)
    next(last_sum)
    w1b, w1w0 = drain(third_sum)
    h01 = mm(w1b, c0_inv, NT)
    h11 = mm(w1w0 - mm(h01, h00, NT), h10_inv, NT)
    a1 = mm(f_inv_low, w1w0, NT)
    right = mm(h01, c0_t, NN) - mm(a1, f_right, TN)
    w1w0_f = mm(w1w0, f_inv, NN)
    a1a1 = mm(a1, a1, TN)
    hh = mm(h01, h01, NT) + mm(h11, h11, NT)
    sol_step = mv1 - mm(mv0, w1w0_f, NT)
    misfit_step = (h01 - mm(w1w0_f, h00, NN), h11 - mm(w1w0_f, h10_t, NT))
    (w1w1,) = drain(last_sum)
    solved, last = factor(with_right(w1w1 - a1a1, identity, right), with_right(w1w1 - hh))
    y_1 = mm(solved[:, 64:96], solved[:, 32:64], TN)
    sol_ref[...] = sol_base + mm(y_1, sol_step, NT)
    misfit_ref[:, :32] = misfit_base[0] - mm(y_1, misfit_step[0], NN)
    misfit_ref[:, 32:64] = misfit_base[1] - mm(y_1, misfit_step[1], NN)
    misfit_ref[:, 64:96] = -mm(y_1, last[:, :32], NT)

    for r in range(3):
        wait_bytes(f1_recv.at[r, pl.ds(0, NB - 1)], send_sem.at[r, 0])
        wait_bytes(f2_recv.at[r, pl.ds(0, NS - 1)], send_sem.at[r, 1])
        if r < 2:
            wait_bytes(f3_recv.at[r, pl.ds(0, NB - 1)], send_sem.at[r, 2])
            wait_bytes(zbuf.at[r, :, pl.ds(0, 31 * ROWS)], z_send_sem.at[r])
    for r, rows in enumerate((8, 16, 16, 8)):
        used = pl.ds(0, rows)
        wait_bytes(ar_x.at[r, pl.ds(0, 3), used], ar_send_sem.at[r, 0])
        wait_bytes(ar_z.at[r, pl.ds(0, 7), used], ar_send_sem.at[r, 1])
        wait_bytes(ar_y.at[r, pl.ds(0, 7), used], ar_send_sem.at[r, 2])
        wait_bytes(ar_core.at[r, pl.ds(0, 1), used], ar_send_sem.at[r, 3])
    wait_bytes(n1_recv.at[pl.ds(0, 248), :], n_send_sem.at[0])
    wait_bytes(n2_recv.at[pl.ds(0, 240), :], n_send_sem.at[1])
    wait_bytes(n1_recv.at[pl.ds(0, 248), :], n_send_sem.at[2])


def body(schur, inverse_blocks, loads, share_list, multiplicity):
    f32 = jnp.float32
    vmem = pl.BlockSpec(memory_space=pltpu.VMEM)
    dma = pltpu.SemaphoreType.DMA
    sol, misfit = pl.pallas_call(
        kernel,
        out_shape=(
            jax.ShapeDtypeStruct((CASES, ROWS), f32),
            jax.ShapeDtypeStruct((CASES, 96), f32),
        ),
        in_specs=[pl.BlockSpec(memory_space=pltpu.SMEM)] * 2
        + [pl.BlockSpec(memory_space=pl.ANY)] * 3,
        out_specs=(vmem, vmem),
        scratch_shapes=[
            pltpu.VMEM((256, 8192), jnp.bfloat16),
            pltpu.VMEM((3, NB, 2, 128), f32),
            pltpu.VMEM((3, NB, 2, 128), f32),
            pltpu.VMEM((3, NS, 4, 128), f32),
            pltpu.VMEM((3, NS, 4, 128), f32),
            pltpu.VMEM((2, NB, 2, 128), f32),
            pltpu.VMEM((2, NB, 2, 128), f32),
            pltpu.VMEM((256, 128), f32),
            pltpu.VMEM((256, 128), f32),
            pltpu.VMEM((256, 128), f32),
            pltpu.VMEM((256, 128), f32),
            pltpu.VMEM((256, 128), f32),
            pltpu.VMEM((256, 128), f32),
            pltpu.VMEM((2, CASES, 8192), jnp.bfloat16),
            pltpu.VMEM((ROWS, CASES), f32),
            pltpu.VMEM((1, CASES, ROWS), f32),
            pltpu.VMEM((1, 2, 128, 128), f32),
            pltpu.VMEM((4, 4, 16, 128), f32),
            pltpu.VMEM((4, 4, 16, 128), f32),
            pltpu.VMEM((4, 8, 16, 128), f32),
            pltpu.VMEM((4, 8, 16, 128), f32),
            pltpu.VMEM((4, 2, 16, 128), f32),
            dma,
            dma((2,)),
            dma((3, 3)),
            dma((3, 3)),
            dma((3,)),
            dma((3,)),
            dma((2,)),
            dma((2, NB)),
            dma((4, 4)),
            dma((4, 4)),
        ],
        compiler_params=pltpu.CompilerParams(collective_id=0, has_side_effects=True),
    )(multiplicity, share_list, loads, inverse_blocks, schur[0])
    return sol[None], misfit


def solution(mesh):
    placed = (
        P("sub", "blk", None),
        P("sub", "blk", None, None),
        P("sub", None, "blk"),
        P("sub", None, None),
        P("sub", "blk"),
    )
    return jax.shard_map(
        body, mesh=mesh, in_specs=placed, out_specs=(P("sub", None, "blk"), P()), check_vma=False
    )
```
